256 devices in a mesh: agents: 64 (over z, x, core), group: 4 (over y).
Axes of the slice: x: 4, y: 4, z: 8, core: 2. Of those that a mesh axis runs over, the one named last changes fastest.
Arguments:
- q_lin: float32 [4, 40, 16384], P('group', None, 'agents'), may hold values from -6 to 6
- inverse: bfloat16 [4, 40, 40, 16384], P('group', None, None, 'agents'), may hold values from -0.5 to 1, as said below
- predict: bfloat16 [4, 40, 40, 16384], P('group', None, None, 'agents'), may hold values from -1 to 1
- free_traj: float32 [4, 40, 16384], P('group', None, 'agents'), may hold values from -6 to 6
- offsets: float32 [4, 8, 40, 16384], P('group', None, None, 'agents'), may hold values from -4 to 4
- multipliers: float32 [4, 8, 40, 16384], P('group', None, None, 'agents'), may hold values from -4 to 4
- nbr_owner: int32 [4, 8, 16384], P('group', None, 'agents'), may hold values from 0 to 63, as said below
- nbr_slot: int32 [4, 8, 16384], P('group', None, 'agents'), may hold values from -1 to 255
- platoon: int32 [4, 16384], P('group', 'agents'), may hold values from 0 to 127, as said below
Outputs:
- inputs_plan: float32 [4, 40, 16384], P('group', None, 'agents')
- multipliers_out: float32 [4, 8, 40, 16384], P('group', None, None, 'agents')
The draws below stay inside these ranges and needn't reach their ends.
Inputs may be any that keep to these rules, and one draw needn't show every extreme that they name: `nbr_owner`: an agent's own block index is its row in the region // 256; each neighbour's owner lies within 2 blocks of it, slot 0 is never padded. `inverse`: symmetric for every agent. `platoon`: 32 or more platoons hold no agent of any region.
All inputs are finite; a program needn't handle non-finite values. Where the reference program divides by a largest or mean magnitude, that divisor is 1e-20 or more.
Results may differ from the reference program's by a relative error of at most 0.0003.
Values sent between devices are 32-bit elements; how exact they have to be, the bound alone decides.
No kernel may reach another device: no remote copies, remote signals or barrier semaphores. Data moves between devices by JAX's collectives and lax.ppermute only.
A program may use at most 64 MiB of HBM per device.

```python
import jax
import jax.numpy as jnp
from jax import lax

A_DEV = 256
QP = 40
TRAJ = 40
DEGREE = 8
SPAN = 2
NPLAT = 128
ITERS = 3
REGIONS = 4
PER = 16384


def neighbour_table(key):
    first, second, third = jax.random.split(jax.random.fold_in(key, 7), 3)
    shape = (REGIONS, DEGREE, PER)
    own = (jnp.arange(PER, dtype=jnp.int32) // A_DEV)[None, None, :]
    step = jax.random.randint(first, shape, -SPAN, SPAN + 1, dtype=jnp.int32)
    owner = jnp.clip(own + step, 0, PER // A_DEV - 1)
    slot = jax.random.randint(second, shape, 0, A_DEV, dtype=jnp.int32)
    alive = jax.random.randint(third, shape, 0, 4, dtype=jnp.int32) > 0
    alive = alive.at[:, 0, :].set(True)
    owner = jnp.where(alive, owner, own + jnp.zeros(shape, jnp.int32))
    slot = jnp.where(alive, slot, -1)
    return (owner, slot)


def draw_nbr_owner(key, part):
    return neighbour_table(key)[0]


def draw_nbr_slot(key, part):
    return neighbour_table(key)[1]


def draw_platoon(key, part):
    order_key, pick_key = jax.random.split(jax.random.fold_in(key, 13))
    order = jax.random.permutation(order_key, NPLAT).astype(jnp.int32)
    used = NPLAT - NPLAT // 4
    index = jax.random.randint(pick_key, (REGIONS, PER), 0, used, dtype=jnp.int32)
    return order[index].astype(jnp.int32)


def draw_inverse(key, part):
    noise_key = jax.random.fold_in(jax.random.fold_in(key, 11), 0)
    base = jax.random.normal(noise_key, (REGIONS, QP, QP, PER), jnp.float32) * 0.07
    sym = 0.5 * (base + jnp.transpose(base, (0, 2, 1, 3)))
    eye = jnp.eye(QP, dtype=jnp.float32)[None, :, :, None]
    whole = 0.5 * eye + sym
    return jnp.clip(whole, -0.5, 1.0).astype(jnp.bfloat16)


def levels(rng, extent, cuts, least, top_value):
    level, own = 1.0, jax.random.fold_in(rng, 6)
    for position, parts in cuts:
        heights = jnp.exp(jax.random.uniform(jax.random.fold_in(own, position), (parts,), jnp.float32, least / len(cuts), top_value / len(cuts)))
        level = level * jnp.repeat(heights, extent[position] // parts).reshape([-1 if axis == position else 1 for axis in range(len(extent))])
    return level


def scatter_about(own_key, extent, spread, most, shards=(), held_as=jnp.bfloat16):
    values = jax.random.normal(own_key, extent, jnp.float32) * spread
    if len(shards) > 0:
        values = levels(own_key, extent, shards, -0.22, 0.18) * values
    return jnp.clip(values, min=-most, max=most).astype(held_as)


def setup_inputs(seed: int = 0) -> dict:
    arg_keys = jax.random.split(jax.random.key(seed), 10)
    q_lin = scatter_about(arg_keys[0], (REGIONS, QP, PER), 1.0, 6.0, ((0, 4), (2, 64)), jnp.float32)
    inverse = draw_inverse(jax.random.fold_in(arg_keys[9], 71), 0)
    predict = scatter_about(arg_keys[2], (REGIONS, TRAJ, QP, PER), QP ** -0.5, 1.0, ((0, 4), (3, 64)))
    free_traj = scatter_about(arg_keys[3], (REGIONS, TRAJ, PER), 1.0, 6.0, ((0, 4), (2, 64)), jnp.float32)
    offsets = scatter_about(arg_keys[4], (REGIONS, DEGREE, TRAJ, PER), 0.5, 4.0, ((0, 4), (3, 64)), jnp.float32)
    multipliers = scatter_about(arg_keys[5], (REGIONS, DEGREE, TRAJ, PER), 0.5, 4.0, ((0, 4), (3, 64)), jnp.float32)
    nbr_owner = draw_nbr_owner(jax.random.fold_in(arg_keys[9], 71), 0)
    nbr_slot = draw_nbr_slot(jax.random.fold_in(arg_keys[9], 71), 0)
    platoon = draw_platoon(jax.random.fold_in(arg_keys[9], 71), 0)
    return {"q_lin": q_lin, "inverse": inverse, "predict": predict, "free_traj": free_traj, "offsets": offsets, "multipliers": multipliers, "nbr_owner": nbr_owner, "nbr_slot": nbr_slot, "platoon": platoon}


RHO = 0.5
KAPPA = 0.5


def lookup(field, nbr_owner, nbr_slot):
    live = nbr_slot >= 0
    column = jnp.where(live, nbr_owner * A_DEV + nbr_slot, 0).astype(jnp.int32)

    def one_region(rows, cols):
        taken = jnp.take(rows, cols.reshape(-1), axis=1)
        return taken.reshape(rows.shape[0], cols.shape[0], cols.shape[1])

    near = jax.vmap(one_region)(field, column)
    near = jnp.transpose(near, (0, 2, 1, 3))
    return near * live[:, :, None, :].astype(jnp.float32)


def platoon_pull(field, onehot):
    sums = jnp.einsum('rta,rpa->tp', field, onehot, precision=lax.Precision.HIGHEST)
    counts = jnp.sum(onehot, axis=(0, 2))
    means = sums / jnp.maximum(counts, 1.0)[None, :]
    return jnp.einsum('tp,rpa->rta', means, onehot, precision=lax.Precision.HIGHEST)


def reference(q_lin, inverse, predict, free_traj, offsets, multipliers, nbr_owner, nbr_slot, platoon):
    live = (nbr_slot >= 0).astype(jnp.float32)[:, :, None, :]
    onehot = (platoon[:, None, :] == jnp.arange(NPLAT, dtype=jnp.int32)[None, :, None]).astype(jnp.float32)
    inverse_wide = inverse.astype(jnp.float32)
    predict_wide = predict.astype(jnp.float32)
    traj = free_traj
    lam = multipliers
    near = lookup(traj, nbr_owner, nbr_slot)
    attract = platoon_pull(traj, onehot)
    plan = jnp.zeros_like(q_lin)
    for step in range(ITERS):
        coupling = jnp.sum(live * (lam - RHO * (near + offsets)), axis=1) - KAPPA * attract
        rhs = q_lin + jnp.einsum('rtja,rta->rja', predict_wide, coupling, precision=lax.Precision.HIGHEST)
        plan = -jnp.einsum('rija,rja->ria', inverse_wide, rhs, precision=lax.Precision.HIGHEST)
        traj = jnp.einsum('rtja,rja->rta', predict_wide, plan, precision=lax.Precision.HIGHEST) + free_traj
        near = lookup(traj, nbr_owner, nbr_slot)
        gap = live * (traj[:, None] - near - offsets)
        peak = jnp.max(jnp.abs(gap))
        lam = lam + gap / (1.0 + peak)
        if step + 1 < ITERS:
            attract = platoon_pull(traj, onehot)
    return plan, lam
```

```python
import functools
import itertools

import jax
import jax.numpy as jnp
from jax import lax
from jax.sharding import Mesh
from jax.sharding import PartitionSpec as P

SPAN = 2
NPLAT = 128
ITERS = 3
AGENTS = ("agents_0", "agents_1", "agents_2")
AGENTS_GROUP = ("agents_0", "agents_1", "agents_2", "group")


RHO = 0.5
KAPPA = 0.5


def shifted(value, axis, steps):
    count = lax.axis_size(axis)
    first, last = (max(0, -steps), min(count, count - steps))
    return lax.ppermute(value, axis, [(source, source + steps) for source in range(first, last)])


def exchanged(value, axes, sources):
    sizes = [lax.axis_size(axis) for axis in axes]
    places = list(itertools.product(*[range(size) for size in sizes]))
    at = {place: k for k, place in enumerate(places)}
    return [value] + [
        lax.ppermute(value, axes, [(at[source(*place)], at[place]) for place in places])
        for source in sources
    ]


def ring(size):
    return [lambda p, k=k: ((p + k) % size,) for k in range(1, size)]


PAIRS = [lambda z, c: (z, 1 - c), lambda z, c: (z ^ 1, c), lambda z, c: (z ^ 1, 1 - c)]
OTHERS = [
    lambda z: ((z - 1 + 2 * (z % 2)) % 8,),
    lambda z: ((z + 2 - 4 * (z % 2)) % 8,),
    lambda z: (z ^ 5,),
]


def joined_all(value, combine):
    stages = (
        (("agents_0", "agents_2"), PAIRS),
        (("agents_0",), OTHERS),
        (("agents_1",), ring(4)),
        (("group",), ring(4)),
    )
    for axes, sources in stages:
        value = combine(exchanged(value, axes, sources))
    return value


def sum_and_peak(pieces):
    row = lax.broadcasted_iota(jnp.int32, pieces[0].shape, 0)
    return jnp.where(
        row < pieces[0].shape[0] - 1, sum(pieces[1:], pieces[0]), functools.reduce(jnp.maximum, pieces)
    )


def added(pieces):
    return sum(pieces[1:], pieces[0])


def local(q_lin, inverse, predict, free_traj, offsets, multipliers, nbr_owner, nbr_slot, platoon):
    block = q_lin.shape[2]
    traj_len = free_traj.shape[1]
    alive = nbr_slot >= 0
    live = alive.astype(jnp.float32)[:, :, None, :]
    onehot = (platoon[:, None, :] == jnp.arange(NPLAT, dtype=jnp.int32)[None, :, None]).astype(
        jnp.float32
    )
    counts_local = jnp.sum(onehot, axis=(0, 2))
    mine = lax.axis_index(AGENTS)
    column = (nbr_owner - mine + SPAN) * block + nbr_slot
    column = jnp.where(alive, column, 0)[0].reshape(-1)

    def lookup(field):
        pieces = []
        for distance in range(-SPAN, SPAN + 1):
            if distance == 0:
                pieces.append(field)
            else:
                pieces.append(shifted(field, AGENTS, -distance))
        joined = jnp.concatenate(pieces, axis=2)
        taken = jnp.take(joined[0], column, axis=1).reshape(traj_len, nbr_slot.shape[1], block)
        return jnp.transpose(taken, (1, 0, 2))[None] * live

    def platoon_local(field):
        return jnp.einsum("rta,rpa->tp", field, onehot, precision=lax.Precision.HIGHEST)

    traj = free_traj
    lam = multipliers
    near = lookup(traj)
    both = joined_all(jnp.concatenate([platoon_local(traj), counts_local[None]]), added)
    sums, counts = both[:traj_len], both[traj_len]
    divisor = jnp.maximum(counts, 1.0)[None, :]

    def spread(totals):
        means = totals / divisor
        return jnp.einsum("tp,rpa->rta", means, onehot, precision=lax.Precision.HIGHEST)

    attract = spread(sums)
    plan = jnp.zeros_like(q_lin)
    for step in range(ITERS):
        coupling = jnp.sum(live * (lam - RHO * (near + offsets)), axis=1) - KAPPA * attract
        rhs = q_lin + jnp.einsum(
            "rtja,rta->rja", predict.astype(jnp.float32), coupling, precision=lax.Precision.HIGHEST
        )
        plan = -jnp.einsum(
            "rija,rja->ria", inverse.astype(jnp.float32), rhs, precision=lax.Precision.HIGHEST
        )
        traj = (
            jnp.einsum(
                "rtja,rja->rta", predict.astype(jnp.float32), plan, precision=lax.Precision.HIGHEST
            )
            + free_traj
        )
        near = lookup(traj)
        gap = live * (traj[:, None] - near - offsets)
        local_peak = jnp.max(jnp.abs(gap))
        more = step + 1 < ITERS
        if more:
            row = jnp.full((1, NPLAT), local_peak)
            both = joined_all(jnp.concatenate([platoon_local(traj), row]), sum_and_peak)
            sums, peak = both[:traj_len], both[traj_len, 0]
        else:
            count = lax.axis_size(AGENTS_GROUP)
            every = jnp.full((count, NPLAT), local_peak)
            peak = jnp.max(lax.all_to_all(every, AGENTS_GROUP, 0, 0, tiled=True))
        lam = lam + gap / (1.0 + peak)
        if more:
            attract = spread(sums)
    return (plan, lam)


def solution(mesh):
    finer = Mesh(
        mesh.devices.reshape(8, 4, 2, mesh.shape["group"]),
        ("agents_0", "agents_1", "agents_2", "group"),
    )
    placed = (
        P("group", None, AGENTS),
        P("group", None, None, AGENTS),
        P("group", None, None, AGENTS),
        P("group", None, AGENTS),
        P("group", None, None, AGENTS),
        P("group", None, None, AGENTS),
        P("group", None, AGENTS),
        P("group", None, AGENTS),
        P("group", AGENTS),
    )
    return jax.shard_map(
        local,
        mesh=finer,
        in_specs=placed,
        out_specs=(P("group", None, AGENTS), P("group", None, None, AGENTS)),
        check_vma=False,
    )
```

```python
import functools
import itertools

import jax
import jax.numpy as jnp
from jax import lax
from jax.experimental import pallas as pl
from jax.experimental.pallas import tpu as pltpu
from jax.sharding import Mesh
from jax.sharding import PartitionSpec as P

SPAN = 2
NPLAT = 128
ITERS = 3
LANES = 128
AGENTS = ("agents_0", "agents_1", "agents_2")
AGENTS_GROUP = ("agents_0", "agents_1", "agents_2", "group")


RHO = 0.5
KAPPA = 0.5


def shifted(value, axis, steps):
    count = lax.axis_size(axis)
    first, last = (max(0, -steps), min(count, count - steps))
    return lax.ppermute(value, axis, [(source, source + steps) for source in range(first, last)])


def exchanged(value, axes, sources):
    sizes = [lax.axis_size(axis) for axis in axes]
    places = list(itertools.product(*[range(size) for size in sizes]))
    at = {place: k for k, place in enumerate(places)}
    return [value] + [
        lax.ppermute(value, axes, [(at[source(*place)], at[place]) for place in places])
        for source in sources
    ]


PAIRS = [lambda z, c: (z, 1 - c), lambda z, c: (z ^ 1, c), lambda z, c: (z ^ 1, 1 - c)]
OTHERS = [
    lambda z: ((z - 1 + 2 * (z % 2)) % 8,),
    lambda z: ((z + 2 - 4 * (z % 2)) % 8,),
    lambda z: (z ^ 5,),
]


def gathered(value, combine):
    value = combine(exchanged(value, ("agents_0", "agents_2"), PAIRS))
    value = combine(exchanged(value, ("agents_0",), OTHERS))
    axes = ("agents_1", "group")
    every = jnp.broadcast_to(value[None], (lax.axis_size(axes), *value.shape))
    return lax.all_to_all(every, axes, 0, 0, tiled=True)


def neighbours(field):
    count = lax.axis_size(AGENTS)
    near = [(k, k + 1 if k % 2 else k - 1) for k in range(count)]
    return (
        field,
        lax.ppermute(field, "agents_2", [(0, 1), (1, 0)]),
        lax.ppermute(field, AGENTS, [(a, b) for a, b in near if 0 <= b < count]),
        shifted(field, AGENTS, 2),
        shifted(field, AGENTS, -2),
    )


def gap_kernel(column, offsets, own, *rest):
    fields, (gap, total, peak) = ((own, *rest[:4]), rest[4:])
    degree, length, block = offsets.shape
    wide = (length, LANES)
    largest = jnp.zeros(wide, jnp.float32)
    for first in range(0, block, LANES):
        here = own[:, first : first + LANES]
        added = jnp.zeros(wide, jnp.float32)
        for k in range(degree):
            index = jnp.broadcast_to(column[k : k + 1, first : first + LANES], wide)
            lane, tile = (index & (LANES - 1), index >> 7)
            near = jnp.zeros(wide, jnp.float32)
            for at in range(len(fields) * block // LANES):
                field = fields[at * LANES // block]
                start = at * LANES % block
                taken = jnp.take_along_axis(
                    field[:, start : start + LANES], lane, axis=1, mode="promise_in_bounds"
                )
                near = jnp.where(tile == at, taken, near)
            value = jnp.where(
                index >= 0, here - near - offsets[k, :, first : first + LANES], 0.0
            )
            gap[k, :, first : first + LANES] = value
            added += value
            largest = jnp.maximum(largest, jnp.abs(value))
        total[:, first : first + LANES] = added
    peak[...] = jnp.broadcast_to(jnp.max(largest), peak.shape)


def gaps(column, offsets, fields, rows):
    degree, length, block = offsets.shape
    return pl.pallas_call(
        gap_kernel,
        out_shape=(
            jax.ShapeDtypeStruct((degree, length, block), jnp.float32),
            jax.ShapeDtypeStruct((length, block), jnp.float32),
            jax.ShapeDtypeStruct((rows, LANES), jnp.float32),
        ),
        compiler_params=pltpu.CompilerParams(vmem_limit_bytes=16 * 1024 * 1024),
        name="gaps",
    )(column, offsets, *fields)


def solve_kernel(first, *refs):
    parts, counts, platoon, q_lin, inverse, predict, free, lam, total, traj, alive = refs[:11]
    plan_out, traj_out, sums_out, scale_out, lam_out = refs[11:]
    length, block = free.shape
    whole = parts[0]
    used = counts[...] > 0.5
    if first:
        for k in range(1, parts.shape[0]):
            whole += parts[k]
        whole = whole[:length]
        scale = jnp.zeros((1, 1), jnp.float32)
    else:
        most = whole
        for k in range(1, parts.shape[0]):
            whole += parts[k]
            most = jnp.maximum(most, parts[k])
        peak = jnp.max(jnp.where(used, 0.0, most), keepdims=True)
        scale = 1.0 / (1.0 + peak)
    means = jnp.where(used, whole, 0.0) / jnp.maximum(counts[...], 1.0)
    onehot = (
        lax.broadcasted_iota(jnp.int32, (NPLAT, block), 0) == platoon[...]
    ).astype(jnp.float32)
    attract = jnp.dot(
        means, onehot, precision=lax.Precision.HIGHEST, preferred_element_type=jnp.float32
    )
    lam_new = lam[...] + scale * total[...] if not first else lam[...]
    coupling = lam_new - RHO * (alive[...] * traj[...] - total[...]) - KAPPA * attract
    rhs = q_lin[...]
    for t in range(length):
        rhs += predict[t].astype(jnp.float32) * coupling[t : t + 1]
    plan = jnp.zeros(rhs.shape, jnp.float32)
    for i in range(rhs.shape[0]):
        plan -= inverse[i].astype(jnp.float32) * rhs[i : i + 1]
    plan_out[...] = plan
    for t in range(length):
        traj_out[t : t + 1] = free[t : t + 1] + jnp.sum(
            predict[t].astype(jnp.float32) * plan, axis=0, keepdims=True
        )
    sums_out[...] = lax.dot_general(
        traj_out[...],
        onehot,
        (((1,), (1,)), ((), ())),
        precision=lax.Precision.HIGHEST,
        preferred_element_type=jnp.float32,
    )
    scale_out[...] = jnp.broadcast_to(scale, scale_out.shape)
    lam_out[...] = lam_new


def solved(first, *args):
    length, block = args[6].shape
    qp = args[3].shape[0]
    return pl.pallas_call(
        functools.partial(solve_kernel, first),
        out_shape=(
            jax.ShapeDtypeStruct((qp, block), jnp.float32),
            jax.ShapeDtypeStruct((length, block), jnp.float32),
            jax.ShapeDtypeStruct((length, NPLAT), jnp.float32),
            jax.ShapeDtypeStruct((8, LANES), jnp.float32),
            jax.ShapeDtypeStruct((length, block), jnp.float32),
        ),
        compiler_params=pltpu.CompilerParams(vmem_limit_bytes=16 * 1024 * 1024),
        name="solve",
    )(*args)


def added(pieces):
    return sum(pieces[1:], pieces[0])


def local(q_lin, inverse, predict, free_traj, offsets, multipliers, nbr_owner, nbr_slot, platoon):
    block = q_lin.shape[2]
    traj_len = free_traj.shape[1]
    q_lin, inverse, predict, free_traj = (q_lin[0], inverse[0], predict[0], free_traj[0])
    offsets, multipliers, owner, slot = (offsets[0], multipliers[0], nbr_owner[0], nbr_slot[0])
    live = slot >= 0
    onehot = (platoon == jnp.arange(NPLAT, dtype=jnp.int32)[:, None]).astype(jnp.float32)
    mine = lax.axis_index(AGENTS)
    away = owner - mine
    beside = jnp.where((away > 0) == (mine % 2 == 0), 1, 2)
    place = jnp.where(away == 0, 0, jnp.where(abs(away) == 1, beside, jnp.where(away < 0, 3, 4)))
    column = jnp.where(live, place * block + slot, -1)
    alive = jnp.sum(live.astype(jnp.float32), axis=0, keepdims=True)
    lam = jnp.sum(jnp.where(live[:, None, :], multipliers, 0.0), axis=0)

    sums = jnp.einsum("ta,pa->tp", free_traj, onehot, precision=lax.Precision.HIGHEST)
    counts = jnp.sum(onehot, axis=1)[None]
    packed = jnp.concatenate([sums, counts, jnp.zeros((7, NPLAT), jnp.float32)])
    parts = gathered(packed, added)
    parts = parts.reshape(-1, *packed.shape)
    counts = jnp.sum(parts[:, traj_len], axis=0, keepdims=True)
    unused = counts < 0.5

    def joined(pieces):
        return jnp.where(unused, functools.reduce(jnp.maximum, pieces), added(pieces))

    traj = free_traj
    _, total, _ = gaps(column, offsets, neighbours(traj), 8)
    new_multipliers = multipliers
    for step in range(ITERS):
        plan, traj, sums, scale, lam = solved(
            step == 0, parts, counts, platoon, q_lin, inverse, predict, free_traj, lam, total, traj, alive
        )
        if step > 0:
            new_multipliers = new_multipliers + scale[0, 0] * gap
        more = step + 1 < ITERS
        count = lax.axis_size(AGENTS_GROUP)
        gap, total, peak = gaps(column, offsets, neighbours(traj), 8 if more else count)
        if more:
            packed = jnp.where(unused, peak[:1], sums)
            parts = gathered(packed, joined).reshape(-1, *packed.shape)
        else:
            peak = jnp.max(lax.all_to_all(peak, AGENTS_GROUP, 0, 0, tiled=True))
            new_multipliers = new_multipliers + gap / (1.0 + peak)
    return (plan[None], new_multipliers[None])


def solution(mesh):
    finer = Mesh(
        mesh.devices.reshape(8, 4, 2, mesh.shape["group"]),
        ("agents_0", "agents_1", "agents_2", "group"),
    )
    placed = (
        P("group", None, AGENTS),
        P("group", None, None, AGENTS),
        P("group", None, None, AGENTS),
        P("group", None, AGENTS),
        P("group", None, None, AGENTS),
        P("group", None, None, AGENTS),
        P("group", None, AGENTS),
        P("group", None, AGENTS),
        P("group", AGENTS),
    )
    return jax.shard_map(
        local,
        mesh=finer,
        in_specs=placed,
        out_specs=(P("group", None, AGENTS), P("group", None, None, AGENTS)),
        check_vma=False,
    )
```

```python
import functools
import itertools

import jax
import jax.numpy as jnp
from jax import lax
from jax.experimental import pallas as pl
from jax.experimental.pallas import tpu as pltpu
from jax.sharding import Mesh
from jax.sharding import PartitionSpec as P

SPAN = 2
NPLAT = 128
ITERS = 3
LANES = 128
AGENTS = ("agents_0", "agents_1", "agents_2")
AGENTS_GROUP = ("agents_0", "agents_1", "agents_2", "group")


RHO = 0.5
KAPPA = 0.5


def shifted(value, axis, steps):
    count = lax.axis_size(axis)
    return lax.ppermute(value, axis, [(source, (source + steps) % count) for source in range(count)])


def exchanged(value, axes, sources):
    sizes = [lax.axis_size(axis) for axis in axes]
    places = list(itertools.product(*[range(size) for size in sizes]))
    at = {place: k for k, place in enumerate(places)}
    return [value] + [
        lax.ppermute(value, axes, [(at[source(*place)], at[place]) for place in places])
        for source in sources
    ]


PAIRS = [lambda z, c: (z, 1 - c), lambda z, c: (z ^ 1, c), lambda z, c: (z ^ 1, 1 - c)]
OTHERS = [
    lambda z: ((z - 1 + 2 * (z % 2)) % 8,),
    lambda z: ((z + 2 - 4 * (z % 2)) % 8,),
    lambda z: (z ^ 5,),
]


def gathered(value, combine, later=None):
    value = combine(exchanged(value, ("agents_0", "agents_2"), PAIRS))
    value = combine(exchanged(value, ("agents_0",), OTHERS))
    if later is not None:
        value, later = lax.optimization_barrier((value, later))
    axes = ("agents_1", "group")
    every = jnp.broadcast_to(value[None], (lax.axis_size(axes), *value.shape))
    return lax.all_to_all(every, axes, 0, 0, tiled=True), later


def neighbours(field):
    count = lax.axis_size(AGENTS)
    near = [(k, (k + 1 if k % 2 else k - 1) % count) for k in range(count)]
    return (
        field,
        lax.ppermute(field, "agents_2", [(0, 1), (1, 0)]),
        lax.ppermute(field, AGENTS, near),
        shifted(field, AGENTS, 2),
        shifted(field, AGENTS, -2),
    )


def gap_kernel(column, offsets, own, *rest):
    fields, (gap, total, peak) = ((own, *rest[:4]), rest[4:])
    degree, length, block = offsets.shape
    wide = (length, LANES)
    largest = jnp.zeros(wide, jnp.float32)
    for first in range(0, block, LANES):
        here = own[:, first : first + LANES]
        added = jnp.zeros(wide, jnp.float32)
        for k in range(degree):
            index = jnp.broadcast_to(column[k : k + 1, first : first + LANES], wide)
            lane, tile = (index & (LANES - 1), index >> 7)
            near = jnp.zeros(wide, jnp.float32)
            for at in range(len(fields) * block // LANES):
                field = fields[at * LANES // block]
                start = at * LANES % block
                taken = jnp.take_along_axis(
                    field[:, start : start + LANES], lane, axis=1, mode="promise_in_bounds"
                )
                near = jnp.where(tile == at, taken, near)
            value = jnp.where(
                index >= 0, here - near - offsets[k, :, first : first + LANES], 0.0
            )
            gap[k, :, first : first + LANES] = value
            added += value
            largest = jnp.maximum(largest, jnp.abs(value))
        total[:, first : first + LANES] = added
    peak[...] = jnp.broadcast_to(jnp.max(largest), peak.shape)


def gaps(column, offsets, fields, rows):
    degree, length, block = offsets.shape
    return pl.pallas_call(
        gap_kernel,
        out_shape=(
            jax.ShapeDtypeStruct((degree, length, block), jnp.float32),
            jax.ShapeDtypeStruct((length, block), jnp.float32),
            jax.ShapeDtypeStruct((rows, LANES), jnp.float32),
        ),
        compiler_params=pltpu.CompilerParams(vmem_limit_bytes=16 * 1024 * 1024),
        name="gaps",
    )(column, offsets, *fields)


def solve_kernel(first, *refs):
    parts, counts, platoon, q_lin, inverse, predict, free, lam, total, traj, alive = refs[:11]
    plan_out, traj_out, sums_out, scale_out, lam_out = refs[11:]
    length, block = free.shape
    whole = parts[0]
    used = counts[...] > 0.5
    if first:
        for k in range(1, parts.shape[0]):
            whole += parts[k]
        whole = whole[:length]
        scale = jnp.zeros((1, 1), jnp.float32)
    else:
        most = whole
        for k in range(1, parts.shape[0]):
            whole += parts[k]
            most = jnp.maximum(most, parts[k])
        peak = jnp.max(jnp.where(used, 0.0, most), keepdims=True)
        scale = 1.0 / (1.0 + peak)
    means = jnp.where(used, whole, 0.0) / jnp.maximum(counts[...], 1.0)
    onehot = (
        lax.broadcasted_iota(jnp.int32, (NPLAT, block), 0) == platoon[...]
    ).astype(jnp.float32)
    attract = jnp.dot(
        means, onehot, precision=lax.Precision.HIGHEST, preferred_element_type=jnp.float32
    )
    lam_new = lam[...] + scale * total[...] if not first else lam[...]
    coupling = lam_new - RHO * (alive[...] * traj[...] - total[...]) - KAPPA * attract
    rhs = q_lin[...]
    for t in range(length):
        rhs += predict[t].astype(jnp.float32) * coupling[t : t + 1]
    plan = jnp.zeros(rhs.shape, jnp.float32)
    for i in range(rhs.shape[0]):
        plan -= inverse[i].astype(jnp.float32) * rhs[i : i + 1]
    plan_out[...] = plan
    for t in range(length):
        traj_out[t : t + 1] = free[t : t + 1] + jnp.sum(
            predict[t].astype(jnp.float32) * plan, axis=0, keepdims=True
        )
    sums_out[...] = lax.dot_general(
        traj_out[...],
        onehot,
        (((1,), (1,)), ((), ())),
        precision=lax.Precision.HIGHEST,
        preferred_element_type=jnp.float32,
    )
    scale_out[...] = jnp.broadcast_to(scale, scale_out.shape)
    lam_out[...] = lam_new


def solved(first, *args):
    length, block = args[6].shape
    qp = args[3].shape[0]
    return pl.pallas_call(
        functools.partial(solve_kernel, first),
        out_shape=(
            jax.ShapeDtypeStruct((qp, block), jnp.float32),
            jax.ShapeDtypeStruct((length, block), jnp.float32),
            jax.ShapeDtypeStruct((length, NPLAT), jnp.float32),
            jax.ShapeDtypeStruct((8, LANES), jnp.float32),
            jax.ShapeDtypeStruct((length, block), jnp.float32),
        ),
        compiler_params=pltpu.CompilerParams(vmem_limit_bytes=16 * 1024 * 1024),
        name="solve",
    )(*args)


def added(pieces):
    return sum(pieces[1:], pieces[0])


def local(q_lin, inverse, predict, free_traj, offsets, multipliers, nbr_owner, nbr_slot, platoon):
    block = q_lin.shape[2]
    traj_len = free_traj.shape[1]
    q_lin, inverse, predict, free_traj = (q_lin[0], inverse[0], predict[0], free_traj[0])
    offsets, multipliers, owner, slot = (offsets[0], multipliers[0], nbr_owner[0], nbr_slot[0])
    live = slot >= 0
    onehot = (platoon == jnp.arange(NPLAT, dtype=jnp.int32)[:, None]).astype(jnp.float32)
    mine = lax.axis_index(AGENTS)
    away = owner - mine
    beside = jnp.where((away > 0) == (mine % 2 == 0), 1, 2)
    place = jnp.where(away == 0, 0, jnp.where(abs(away) == 1, beside, jnp.where(away < 0, 3, 4)))
    column = jnp.where(live, place * block + slot, -1)
    alive = jnp.sum(live.astype(jnp.float32), axis=0, keepdims=True)
    lam = jnp.sum(jnp.where(live[:, None, :], multipliers, 0.0), axis=0)

    sums = jnp.einsum("ta,pa->tp", free_traj, onehot, precision=lax.Precision.HIGHEST)
    counts = jnp.sum(onehot, axis=1)[None]
    packed = jnp.concatenate([sums, counts, jnp.zeros((7, NPLAT), jnp.float32)])
    parts, traj = gathered(packed, added, free_traj)
    parts = parts.reshape(-1, *packed.shape)
    counts = jnp.sum(parts[:, traj_len], axis=0, keepdims=True)
    unused = counts < 0.5

    def joined(pieces):
        return jnp.where(unused, functools.reduce(jnp.maximum, pieces), added(pieces))

    _, total, _ = gaps(column, offsets, neighbours(traj), 8)
    new_multipliers = multipliers
    for step in range(ITERS):
        plan, traj, sums, scale, lam = solved(
            step == 0, parts, counts, platoon, q_lin, inverse, predict, free_traj, lam, total, traj, alive
        )
        if step > 0:
            new_multipliers = new_multipliers + scale[0, 0] * gap
        more = step + 1 < ITERS
        count = lax.axis_size(AGENTS_GROUP)
        gap, total, peak = gaps(column, offsets, neighbours(traj), 8 if more else count)
        if more:
            packed = jnp.where(unused, peak[:1], sums)
            parts = gathered(packed, joined)[0].reshape(-1, *packed.shape)
        else:
            peak = jnp.max(lax.all_to_all(peak, AGENTS_GROUP, 0, 0, tiled=True))
            new_multipliers = new_multipliers + gap / (1.0 + peak)
    return (plan[None], new_multipliers[None])


def solution(mesh):
    finer = Mesh(
        mesh.devices.reshape(8, 4, 2, mesh.shape["group"]),
        ("agents_0", "agents_1", "agents_2", "group"),
    )
    placed = (
        P("group", None, AGENTS),
        P("group", None, None, AGENTS),
        P("group", None, None, AGENTS),
        P("group", None, AGENTS),
        P("group", None, None, AGENTS),
        P("group", None, None, AGENTS),
        P("group", None, AGENTS),
        P("group", None, AGENTS),
        P("group", AGENTS),
    )
    return jax.shard_map(
        local,
        mesh=finer,
        in_specs=placed,
        out_specs=(P("group", None, AGENTS), P("group", None, None, AGENTS)),
        check_vma=False,
    )
```

```python
import functools
import itertools

import jax
import jax.numpy as jnp
from jax import lax
from jax.experimental import pallas as pl
from jax.experimental.pallas import tpu as pltpu
from jax.sharding import Mesh
from jax.sharding import PartitionSpec as P

NPLAT = 128
ITERS = 3
LANES = 128
AGENTS = ("agents_0", "agents_1", "agents_2")
AGENTS_GROUP = ("agents_0", "agents_1", "agents_2", "group")


RHO = 0.5
KAPPA = 0.5


def shifted(value, axis, steps):
    count = lax.axis_size(axis)
    return lax.ppermute(value, axis, [(source, (source + steps) % count) for source in range(count)])


def exchanged(value, axes, sources):
    sizes = [lax.axis_size(axis) for axis in axes]
    places = list(itertools.product(*[range(size) for size in sizes]))
    at = {place: k for k, place in enumerate(places)}
    return [value] + [
        lax.ppermute(value, axes, [(at[source(*place)], at[place]) for place in places])
        for source in sources
    ]


PAIRS = [lambda z, c: (z, 1 - c), lambda z, c: (z ^ 1, c), lambda z, c: (z ^ 1, 1 - c)]
OTHERS = [
    lambda z: ((z - 1 + 2 * (z % 2)) % 8,),
    lambda z: ((z + 2 - 4 * (z % 2)) % 8,),
    lambda z: (z ^ 5,),
]


def gathered(value, combine, ready=None):
    value = combine(exchanged(value, ("agents_0", "agents_2"), PAIRS))
    value = combine(exchanged(value, ("agents_0",), OTHERS))
    if ready is not None:
        value, ready = lax.optimization_barrier((value, ready))
    axes = ("agents_1", "group")
    every = jnp.broadcast_to(value[None], (lax.axis_size(axes), *value.shape))
    return lax.all_to_all(every, axes, 0, 0, tiled=True), ready


def neighbours(field):
    count = lax.axis_size(AGENTS)
    near = [(k, (k + 1 if k % 2 else k - 1) % count) for k in range(count)]
    return (
        field,
        lax.ppermute(field, "agents_2", [(0, 1), (1, 0)]),
        lax.ppermute(field, AGENTS, near),
        shifted(field, AGENTS, 2),
        shifted(field, AGENTS, -2),
    )


def gap_kernel(column, offsets, own, *rest):
    fields, (total, *kept) = ((own, *rest[:4]), rest[4:])
    degree, length, block = offsets.shape
    wide = (length, LANES)
    largest = jnp.zeros(wide, jnp.float32)
    for first in range(0, block, LANES):
        here = own[:, first : first + LANES]
        added = jnp.zeros(wide, jnp.float32)
        for k in range(degree):
            index = jnp.broadcast_to(column[k : k + 1, first : first + LANES], wide)
            lane, tile = (index & (LANES - 1), index >> 7)
            near = jnp.zeros(wide, jnp.float32)
            for at in range(len(fields) * block // LANES):
                field = fields[at * LANES // block]
                start = at * LANES % block
                taken = jnp.take_along_axis(
                    field[:, start : start + LANES], lane, axis=1, mode="promise_in_bounds"
                )
                near = jnp.where(tile == at, taken, near)
            value = jnp.where(
                index >= 0, here - near - offsets[k, :, first : first + LANES], 0.0
            )
            added += value
            if kept:
                kept[0][k, :, first : first + LANES] = value
                largest = jnp.maximum(largest, jnp.abs(value))
        total[:, first : first + LANES] = added
    if kept:
        kept[1][...] = jnp.broadcast_to(jnp.max(largest), kept[1].shape)


def gaps(column, offsets, fields, rows):
    degree, length, block = offsets.shape
    shapes = [(length, block), (degree, length, block), (rows, LANES)]
    return pl.pallas_call(
        gap_kernel,
        out_shape=[
            jax.ShapeDtypeStruct(shape, jnp.float32) for shape in shapes[: 3 if rows else 1]
        ],
        compiler_params=pltpu.CompilerParams(vmem_limit_bytes=16 * 1024 * 1024),
        name="gaps",
    )(column, offsets, *fields)


def solve_kernel(first, *refs):
    parts, counts, platoon, q_lin, inverse, predict, free, lam, total, traj, alive = refs[:11]
    plan_out, traj_out, sums_out, scale_out, lam_out = refs[11:]
    length, block = free.shape
    whole = parts[0]
    used = counts[...] > 0.5
    if first:
        for k in range(1, parts.shape[0]):
            whole += parts[k]
        whole = whole[:length]
        scale = jnp.zeros((1, 1), jnp.float32)
    else:
        most = whole
        for k in range(1, parts.shape[0]):
            whole += parts[k]
            most = jnp.maximum(most, parts[k])
        peak = jnp.max(jnp.where(used, 0.0, most), keepdims=True)
        scale = 1.0 / (1.0 + peak)
    means = jnp.where(used, whole, 0.0) / jnp.maximum(counts[...], 1.0)
    onehot = (
        lax.broadcasted_iota(jnp.int32, (NPLAT, block), 0) == platoon[...]
    ).astype(jnp.float32)
    attract = jnp.dot(
        means, onehot, precision=lax.Precision.HIGHEST, preferred_element_type=jnp.float32
    )
    lam_new = lam[...] + scale * total[...] if not first else lam[...]
    coupling = lam_new - RHO * (alive[...] * traj[...] - total[...]) - KAPPA * attract
    rhs = q_lin[...]
    for t in range(length):
        rhs += predict[t].astype(jnp.float32) * coupling[t : t + 1]
    plan = jnp.zeros(rhs.shape, jnp.float32)
    for i in range(rhs.shape[0]):
        plan -= inverse[i].astype(jnp.float32) * rhs[i : i + 1]
    plan_out[...] = plan
    for t in range(length):
        traj_out[t : t + 1] = free[t : t + 1] + jnp.sum(
            predict[t].astype(jnp.float32) * plan, axis=0, keepdims=True
        )
    sums_out[...] = lax.dot_general(
        traj_out[...],
        onehot,
        (((1,), (1,)), ((), ())),
        precision=lax.Precision.HIGHEST,
        preferred_element_type=jnp.float32,
    )
    scale_out[...] = jnp.broadcast_to(scale, scale_out.shape)
    lam_out[...] = lam_new


def solved(first, *args):
    length, block = args[6].shape
    qp = args[3].shape[0]
    return pl.pallas_call(
        functools.partial(solve_kernel, first),
        out_shape=(
            jax.ShapeDtypeStruct((qp, block), jnp.float32),
            jax.ShapeDtypeStruct((length, block), jnp.float32),
            jax.ShapeDtypeStruct((length, NPLAT), jnp.float32),
            jax.ShapeDtypeStruct((length, block), jnp.float32),
            jax.ShapeDtypeStruct((length, block), jnp.float32),
        ),
        compiler_params=pltpu.CompilerParams(vmem_limit_bytes=16 * 1024 * 1024),
        name="solve",
    )(*args)


def finish_kernel(peaks, before, gap, out):
    out[...] = before[...] + gap[...] * (1.0 / (1.0 + jnp.max(peaks[...])))


def finished(peaks, before, gap):
    return pl.pallas_call(
        finish_kernel,
        out_shape=jax.ShapeDtypeStruct(gap.shape, jnp.float32),
        compiler_params=pltpu.CompilerParams(vmem_limit_bytes=16 * 1024 * 1024),
        name="finish",
    )(peaks, before, gap)


def added(pieces):
    return sum(pieces[1:], pieces[0])


def local(q_lin, inverse, predict, free_traj, offsets, multipliers, nbr_owner, nbr_slot, platoon):
    block = q_lin.shape[2]
    traj_len = free_traj.shape[1]
    q_lin, inverse, predict, free_traj = (q_lin[0], inverse[0], predict[0], free_traj[0])
    offsets, multipliers, owner, slot = (offsets[0], multipliers[0], nbr_owner[0], nbr_slot[0])
    live = slot >= 0
    onehot = (platoon == jnp.arange(NPLAT, dtype=jnp.int32)[:, None]).astype(jnp.float32)
    mine = lax.axis_index(AGENTS)
    away = owner - mine
    beside = jnp.where((away > 0) == (mine % 2 == 0), 1, 2)
    place = jnp.where(away == 0, 0, jnp.where(abs(away) == 1, beside, jnp.where(away < 0, 3, 4)))
    column = jnp.where(live, place * block + slot, -1)
    alive = jnp.sum(live.astype(jnp.float32), axis=0, keepdims=True)
    lam = jnp.sum(jnp.where(live[:, None, :], multipliers, 0.0), axis=0)

    sums = jnp.einsum("ta,pa->tp", free_traj, onehot, precision=lax.Precision.HIGHEST)
    counts = jnp.sum(onehot, axis=1)[None]
    packed = jnp.concatenate([sums, counts, jnp.zeros((7, NPLAT), jnp.float32)])
    fields = neighbours(free_traj)
    (total,) = gaps(column, offsets, fields, 0)
    parts, (total, lam, column, alive) = gathered(packed, added, (total, lam, column, alive))
    traj = free_traj
    parts = parts.reshape(-1, *packed.shape)
    counts = jnp.sum(parts[:, traj_len], axis=0, keepdims=True)
    unused = counts < 0.5

    def joined(pieces):
        return jnp.where(unused, functools.reduce(jnp.maximum, pieces), added(pieces))

    new_multipliers = multipliers
    for step in range(ITERS):
        plan, traj, sums, scale, lam = solved(
            step == 0, parts, counts, platoon, q_lin, inverse, predict, free_traj, lam, total, traj, alive
        )
        if step > 0:
            new_multipliers = new_multipliers + scale[None] * gap
        more = step + 1 < ITERS
        count = lax.axis_size(AGENTS_GROUP)
        total, gap, peak = gaps(column, offsets, neighbours(traj), 8 if more else count)
        if more:
            packed = jnp.where(unused, peak[:1], sums)
            parts = gathered(packed, joined)[0].reshape(-1, *packed.shape)
        else:
            peak, new_multipliers = lax.optimization_barrier((peak, new_multipliers))
            peaks = lax.all_to_all(peak, AGENTS_GROUP, 0, 0, tiled=True)
            new_multipliers = finished(peaks, new_multipliers, gap)
    return (plan[None], new_multipliers[None])


def solution(mesh):
    finer = Mesh(
        mesh.devices.reshape(8, 4, 2, mesh.shape["group"]),
        ("agents_0", "agents_1", "agents_2", "group"),
    )
    placed = (
        P("group", None, AGENTS),
        P("group", None, None, AGENTS),
        P("group", None, None, AGENTS),
        P("group", None, AGENTS),
        P("group", None, None, AGENTS),
        P("group", None, None, AGENTS),
        P("group", None, AGENTS),
        P("group", None, AGENTS),
        P("group", AGENTS),
    )
    return jax.shard_map(
        local,
        mesh=finer,
        in_specs=placed,
        out_specs=(P("group", None, AGENTS), P("group", None, None, AGENTS)),
        check_vma=False,
    )
```

```python
import functools
import itertools

import jax
import jax.numpy as jnp
from jax import lax
from jax.experimental import pallas as pl
from jax.experimental.pallas import tpu as pltpu
from jax.sharding import Mesh
from jax.sharding import PartitionSpec as P

NPLAT = 128
ITERS = 3
LANES = 128
AGENTS = ("agents_0", "agents_1", "agents_2")
AGENTS_GROUP = ("agents_0", "agents_1", "agents_2", "group")


RHO = 0.5
KAPPA = 0.5


def shifted(value, axis, steps):
    count = lax.axis_size(axis)
    return lax.ppermute(value, axis, [(source, (source + steps) % count) for source in range(count)])


def exchanged(value, axes, sources):
    sizes = [lax.axis_size(axis) for axis in axes]
    places = list(itertools.product(*[range(size) for size in sizes]))
    at = {place: k for k, place in enumerate(places)}
    return [value] + [
        lax.ppermute(value, axes, [(at[source(*place)], at[place]) for place in places])
        for source in sources
    ]


PAIRS = [lambda z, c: (z, 1 - c), lambda z, c: (z ^ 1, c), lambda z, c: (z ^ 1, 1 - c)]
OTHERS = [
    lambda z: ((z - 1 + 2 * (z % 2)) % 8,),
    lambda z: ((z + 2 - 4 * (z % 2)) % 8,),
    lambda z: (z ^ 5,),
]


def gathered(value, combine, ready=None):
    value = combine(exchanged(value, ("agents_0", "agents_2"), PAIRS))
    value = combine(exchanged(value, ("agents_0",), OTHERS))
    if ready is not None:
        value, ready = lax.optimization_barrier((value, ready))
    axes = ("agents_1", "group")
    every = jnp.broadcast_to(value[None], (lax.axis_size(axes), *value.shape))
    return lax.all_to_all(every, axes, 0, 0, tiled=True), ready


def neighbours(field):
    count = lax.axis_size(AGENTS)
    near = [(k, (k + 1 if k % 2 else k - 1) % count) for k in range(count)]
    return (
        field,
        lax.ppermute(field, "agents_2", [(0, 1), (1, 0)]),
        lax.ppermute(field, AGENTS, near),
        shifted(field, AGENTS, 2),
        shifted(field, AGENTS, -2),
    )


def gap_kernel(summed, column, offsets, own, *rest):
    fields, outs = ((own, *rest[:4]), list(rest[4:]))
    total = outs.pop(0) if summed else None
    degree, length, block = offsets.shape
    wide = (length, LANES)
    largest = jnp.zeros(wide, jnp.float32)
    for first in range(0, block, LANES):
        here = own[:, first : first + LANES]
        added = jnp.zeros(wide, jnp.float32)
        for k in range(degree):
            index = jnp.broadcast_to(column[k : k + 1, first : first + LANES], wide)
            lane, tile = (index & (LANES - 1), index >> 7)
            near = jnp.zeros(wide, jnp.float32)
            for at in range(len(fields) * block // LANES):
                field = fields[at * LANES // block]
                start = at * LANES % block
                taken = jnp.take_along_axis(
                    field[:, start : start + LANES], lane, axis=1, mode="promise_in_bounds"
                )
                near = jnp.where(tile == at, taken, near)
            value = jnp.where(
                index >= 0, here - near - offsets[k, :, first : first + LANES], 0.0
            )
            added += value
            if outs:
                outs[0][k, :, first : first + LANES] = value
                largest = jnp.maximum(largest, jnp.abs(value))
        if summed:
            total[:, first : first + LANES] = added
    if outs:
        outs[1][...] = jnp.broadcast_to(jnp.max(largest), outs[1].shape)


def gaps(column, offsets, fields, summed, kept):
    degree, length, block = offsets.shape
    shapes = [(length, block)] * summed + [(degree, length, block), (8, LANES)] * kept
    return pl.pallas_call(
        functools.partial(gap_kernel, summed),
        out_shape=[jax.ShapeDtypeStruct(shape, jnp.float32) for shape in shapes],
        compiler_params=pltpu.CompilerParams(vmem_limit_bytes=16 * 1024 * 1024),
        name="gaps",
    )(column, offsets, *fields)


def picked(value, onehot, contract):
    rows, pieces = (value.shape[0], [])
    for _ in range(3):
        pieces.append(value.astype(jnp.bfloat16))
        value = value - pieces[-1].astype(jnp.float32)
    out = lax.dot_general(
        jnp.concatenate(pieces, axis=0),
        onehot,
        (((1,), (contract,)), ((), ())),
        preferred_element_type=jnp.float32,
    )
    return out[:rows] + out[rows : 2 * rows] + out[2 * rows :]


def solve_kernel(first, last, *refs):
    parts, counts, platoon, q_lin, inverse, predict, free, lam, total, traj, alive = refs[:11]
    traj_out, *others = refs[11:]
    length, block = free.shape
    whole = parts[0]
    used = counts[...] > 0.5
    if first:
        for k in range(1, parts.shape[0]):
            whole += parts[k]
        whole = whole[:length]
        scale = jnp.zeros((1, 1), jnp.float32)
    else:
        most = whole
        for k in range(1, parts.shape[0]):
            whole += parts[k]
            most = jnp.maximum(most, parts[k])
        peak = jnp.max(jnp.where(used, 0.0, most), keepdims=True)
        scale = 1.0 / (1.0 + peak)
    means = jnp.where(used, whole, 0.0) / jnp.maximum(counts[...], 1.0)
    onehot = (
        lax.broadcasted_iota(jnp.int32, (NPLAT, block), 0) == platoon[...]
    ).astype(jnp.bfloat16)
    attract = picked(means, onehot, 0)
    lam_new = lam[...] + scale * total[...] if not first else lam[...]
    coupling = lam_new - RHO * (alive[...] * traj[...] - total[...]) - KAPPA * attract
    rhs = q_lin[...]
    for t in range(length):
        rhs += predict[t].astype(jnp.float32) * coupling[t : t + 1]
    plan = jnp.zeros(rhs.shape, jnp.float32)
    for i in range(rhs.shape[0]):
        plan -= inverse[i].astype(jnp.float32) * rhs[i : i + 1]
    for t in range(length):
        traj_out[t : t + 1] = free[t : t + 1] + jnp.sum(
            predict[t].astype(jnp.float32) * plan, axis=0, keepdims=True
        )
    if last:
        others[0][...] = plan
    else:
        others[0][...] = picked(traj_out[...], onehot, 1)
        others[1][...] = lam_new
    if not first:
        others[-1][...] = jnp.broadcast_to(scale, others[-1].shape)


def solved(first, last, *args):
    length, block = args[6].shape
    shapes = [(length, block)] + ([args[3].shape] if last else [(length, NPLAT), (length, block)])
    shapes += [] if first else [(length, block)]
    return pl.pallas_call(
        functools.partial(solve_kernel, first, last),
        out_shape=[jax.ShapeDtypeStruct(shape, jnp.float32) for shape in shapes],
        compiler_params=pltpu.CompilerParams(vmem_limit_bytes=16 * 1024 * 1024),
        name="solve",
    )(*args)


def finish_kernel(peaks, before, gap, plan, out, plan_out):
    plan_out[...] = plan[...]
    out[...] = before[...] + gap[...] * (1.0 / (1.0 + jnp.max(peaks[...])))


def finished(peaks, before, gap, plan):
    return pl.pallas_call(
        finish_kernel,
        out_shape=[jax.ShapeDtypeStruct(x.shape, jnp.float32) for x in (gap, plan)],
        compiler_params=pltpu.CompilerParams(vmem_limit_bytes=16 * 1024 * 1024),
        name="finish",
    )(peaks, before, gap, plan)


def added(pieces):
    return sum(pieces[1:], pieces[0])


def local(q_lin, inverse, predict, free_traj, offsets, multipliers, nbr_owner, nbr_slot, platoon):
    block = q_lin.shape[2]
    traj_len = free_traj.shape[1]
    q_lin, inverse, predict, free_traj = (q_lin[0], inverse[0], predict[0], free_traj[0])
    offsets, multipliers, owner, slot = (offsets[0], multipliers[0], nbr_owner[0], nbr_slot[0])
    live = slot >= 0
    onehot = (platoon == jnp.arange(NPLAT, dtype=jnp.int32)[:, None]).astype(jnp.float32)
    mine = lax.axis_index(AGENTS)
    away = owner - mine
    beside = jnp.where((away > 0) == (mine % 2 == 0), 1, 2)
    place = jnp.where(away == 0, 0, jnp.where(abs(away) == 1, beside, jnp.where(away < 0, 3, 4)))
    column = jnp.where(live, place * block + slot, -1)
    alive = jnp.sum(live.astype(jnp.float32), axis=0, keepdims=True)
    lam = jnp.sum(jnp.where(live[:, None, :], multipliers, 0.0), axis=0)

    sums = jnp.einsum("ta,pa->tp", free_traj, onehot, precision=lax.Precision.HIGHEST)
    counts = jnp.sum(onehot, axis=1)[None]
    packed = jnp.concatenate([sums, counts, jnp.zeros((7, NPLAT), jnp.float32)])
    fields = neighbours(free_traj)
    (total,) = gaps(column, offsets, fields, True, False)
    parts, (total, lam, column, alive) = gathered(packed, added, (total, lam, column, alive))
    traj = free_traj
    parts = parts.reshape(-1, *packed.shape)
    counts = jnp.sum(parts[:, traj_len], axis=0, keepdims=True)
    unused = counts < 0.5

    def joined(pieces):
        return jnp.where(unused, functools.reduce(jnp.maximum, pieces), added(pieces))

    new_multipliers = multipliers
    for step in range(ITERS):
        more = step + 1 < ITERS
        args = (q_lin, inverse, predict, free_traj, lam, total, traj, alive)
        traj, *others = solved(step == 0, not more, parts, counts, platoon, *args)
        if step > 0:
            new_multipliers = new_multipliers + others.pop()[None] * gap
        *sums_of, gap, peak = gaps(column, offsets, neighbours(traj), more, True)
        if more:
            (total,), (sums, lam) = (sums_of, others)
            packed = jnp.where(unused, peak[:1], sums)
            parts = gathered(packed, joined)[0].reshape(-1, *packed.shape)
        else:
            peak = jnp.broadcast_to(peak[:1], (lax.axis_size(AGENTS_GROUP), LANES))
            peak, new_multipliers = lax.optimization_barrier((peak, new_multipliers))
            peaks = lax.all_to_all(peak, AGENTS_GROUP, 0, 0, tiled=True)
            new_multipliers, plan = finished(peaks, new_multipliers, gap, others[0])
    return (plan[None], new_multipliers[None])


def solution(mesh):
    finer = Mesh(
        mesh.devices.reshape(8, 4, 2, mesh.shape["group"]),
        ("agents_0", "agents_1", "agents_2", "group"),
    )
    placed = (
        P("group", None, AGENTS),
        P("group", None, None, AGENTS),
        P("group", None, None, AGENTS),
        P("group", None, AGENTS),
        P("group", None, None, AGENTS),
        P("group", None, None, AGENTS),
        P("group", None, AGENTS),
        P("group", None, AGENTS),
        P("group", AGENTS),
    )
    return jax.shard_map(
        local,
        mesh=finer,
        in_specs=placed,
        out_specs=(P("group", None, AGENTS), P("group", None, None, AGENTS)),
        check_vma=False,
    )
```
